64 devices in a mesh: dp: 8 (over x, y, core), tp: 8 (over z).
Axes of the slice: x: 2, y: 2, z: 8, core: 2. Of those that a mesh axis runs over, the one named last changes fastest.
The devices are a block of a 4x4x8 slice.
Arguments:
- x: bfloat16 [16384, 3584], P('dp'), parts along dimension 0
- w_gate: bfloat16 [3584, 14336], P(None, 'tp')
- w_up: bfloat16 [3584, 14336], P(None, 'tp')
- w_down: bfloat16 [14336, 3584], P('tp')
Outputs:
- output: bfloat16 [16384, 3584], P('dp'), parts along dimension 0
There are 8 independent parts. The reference program is written for one: setup_inputs(seed, part) draws one part's arguments, and reference() takes and returns one part's arrays. A program takes and returns all parts, laid end to end along the dimension named above; an argument that names none is the same for every part.
All inputs are finite; a program needn't handle non-finite values.
Results may differ from the reference program's by a relative error of at most 0.016.
Values are sent between devices in bfloat16 or wider.
A program may use at most 768 MiB of HBM per device.

```python
import jax
import jax.numpy as jnp

ROWS = 2048
D = 3584
FF = 14336


def setup_inputs(seed: int = 0, part: int = 0) -> dict:
    kx, kg, ku, kd = jax.random.split(jax.random.key(seed), 4)
    drawn = {
        "x": jax.random.normal(jax.random.fold_in(kx, part), (ROWS, D), jnp.float32),
        "w_gate": jax.random.normal(kg, (D, FF), jnp.float32) * D**-0.5,
        "w_up": jax.random.normal(ku, (D, FF), jnp.float32) * D**-0.5,
        "w_down": jax.random.normal(kd, (FF, D), jnp.float32) * FF**-0.5,
    }
    return {k: v.astype(jnp.bfloat16) for k, v in drawn.items()}


def reference(x, w_gate, w_up, w_down):
    gate = jnp.dot(x, w_gate, preferred_element_type=jnp.float32)
    up = jnp.dot(x, w_up, preferred_element_type=jnp.float32)
    hidden = (jax.nn.gelu(gate) * up).astype(jnp.bfloat16)
    return jnp.dot(hidden, w_down, preferred_element_type=jnp.float32).astype(jnp.bfloat16)
```

```python
import functools

import jax
import jax.numpy as jnp
from jax import lax
from jax.experimental import pallas as pl
from jax.experimental.pallas import tpu as pltpu
from jax.sharding import PartitionSpec as P

MESH = pl.DeviceIdType.MESH
PIECES = 7
CW, CCW = 0, 1


def kernel(n, x_hbm, wg_hbm, wu_hbm, wd_hbm, y_hbm, wgu, wd, xb, hid, buf,
           wgu_sem, wd_sem, x_sem, rs_recv, ag_recv, rs_send, ag_send, own_sem):
    me = lax.axis_index("tp")
    right, left = lax.rem(me + 1, n), lax.rem(me + n - 1, n)
    target = ({"tp": right}, {"tp": left})
    chunk = x_hbm.shape[0] // n
    half = chunk // 2
    fb = wgu.shape[2] // 2
    db = wd.shape[2]

    def rows(d, c):
        return pl.ds(pl.multiple_of(c * chunk + d * half, half), half)

    def rs_chunk(d, k):
        return lax.rem(me + (2 * n - 1 - k if d == CW else 1 + k), n)

    def ag_chunk(d, m):
        return lax.rem(me + (2 * n - m if d == CW else m), n)

    def cols(j):
        return pl.ds(pl.multiple_of(j * db, db), db)

    def x_copy(d, k):
        slot = lax.rem(k, 2)
        return pltpu.make_async_copy(
            x_hbm.at[rows(d, rs_chunk(d, k))], xb.at[slot, pl.ds(d * half, half)], x_sem.at[slot, d])

    def gu_copies(j):
        c = pl.ds(pl.multiple_of(j * fb, fb), fb)
        return (pltpu.make_async_copy(wg_hbm.at[:, c], wgu.at[j, :, pl.ds(0, fb)], wgu_sem.at[0, j]),
                pltpu.make_async_copy(wu_hbm.at[:, c], wgu.at[j, :, pl.ds(fb, fb)], wgu_sem.at[1, j]))

    def wd_copy(j):
        return pltpu.make_async_copy(wd_hbm.at[:, cols(j)], wd.at[j], wd_sem.at[j])

    def rs_copy(d, k, j):
        return pltpu.make_async_remote_copy(
            src_ref=buf.at[d, k, j], dst_ref=buf.at[d, k + 1, j],
            send_sem=rs_send.at[d], recv_sem=rs_recv.at[d, k + 1, j],
            device_id=target[d], device_id_type=MESH)

    def rs_wait(d, k, j):
        pltpu.make_async_copy(buf.at[d, k, j], buf.at[d, k, j], rs_recv.at[d, k, j]).wait()

    def y_piece(d, m, j):
        return y_hbm.at[rows(d, ag_chunk(d, m)), cols(j)]

    def ag_copy(d, m, j, src):
        return pltpu.make_async_remote_copy(
            src_ref=src, dst_ref=y_piece(d, m, j),
            send_sem=ag_send.at[d], recv_sem=ag_recv.at[d, m + 1, j],
            device_id=target[d], device_id_type=MESH)

    def own_copy(d, j):
        return pltpu.make_async_copy(buf.at[d, n - 1, j], y_piece(d, 0, j), own_sem.at[d, j])

    def gate_up(slot, j):
        gu = jnp.dot(xb[slot], wgu[j], preferred_element_type=jnp.float32)
        h = jax.nn.gelu(gu[:, :fb]) * gu[:, fb:]
        hid[slot, :, pl.ds(pl.multiple_of(j * fb, fb), fb)] = h.astype(hid.dtype)

    def down(k, j, first):
        acc = jnp.dot(hid[lax.rem(k, 2)], wd[j], preferred_element_type=jnp.float32)
        for d in (CW, CCW):
            part = acc[d * half:(d + 1) * half]
            if not first:
                rs_wait(d, k, j)
                part = part + buf[d, k, j].astype(jnp.float32)
            buf[d, k, j] = part.astype(buf.dtype)

    for d in (CW, CCW):
        x_copy(d, 0).start()
    for j in range(PIECES):
        for c in gu_copies(j):
            c.start()
    for j in range(PIECES):
        wd_copy(j).start()
    for d in (CW, CCW):
        x_copy(d, 1).start()
    barrier = pltpu.get_barrier_semaphore()
    for d in (CW, CCW):
        pl.semaphore_signal(barrier, inc=1, device_id=target[d], device_id_type=MESH)

    for d in (CW, CCW):
        x_copy(d, 0).wait()

    def prologue(j, _):
        for c in gu_copies(j):
            c.wait()
        gate_up(0, j)
        return 0

    lax.fori_loop(0, PIECES, prologue, 0)
    pl.semaphore_wait(barrier, 2)

    def step(k, first):
        nxt = lax.rem(k + 1, 2)
        for d in (CW, CCW):
            x_copy(d, k + 1).wait()

        def piece(j, _):
            if first:
                wd_copy(j).wait()
            down(k, j, first)
            for d in (CW, CCW):
                rs_copy(d, k, j).start()
            gate_up(nxt, j)
            return 0

        lax.fori_loop(0, PIECES, piece, 0)

    step(0, True)

    def middle(k, _):
        for d in (CW, CCW):
            x_copy(d, k + 1).start()
        step(k, False)
        return 0

    lax.fori_loop(1, n - 1, middle, 0)

    def last(j, _):
        down(n - 1, j, False)
        for d in (CW, CCW):
            ag_copy(d, 0, j, buf.at[d, n - 1, j]).start()
            own_copy(d, j).start()
        return 0

    lax.fori_loop(0, PIECES, last, 0)

    def ag_wait(d, m, j):
        pltpu.make_async_copy(y_piece(d, m, j), y_piece(d, m, j), ag_recv.at[d, m, j]).wait()

    def gather(m, forward):
        def piece(j, _):
            for d in (CW, CCW):
                ag_wait(d, m, j)
                if forward:
                    ag_copy(d, m, j, y_piece(d, m, j)).start()
            return 0

        lax.fori_loop(0, PIECES, piece, 0)

    def gather_forward(m, _):
        gather(m, True)
        return 0

    lax.fori_loop(1, n - 1, gather_forward, 0)
    gather(n - 1, False)

    for d in (CW, CCW):
        sent = buf.at[d, pl.ds(0, n - 1)]
        pltpu.make_async_copy(sent, sent, rs_send.at[d]).wait()
        sent = y_hbm.at[pl.ds(0, (n - 1) * half)]
        pltpu.make_async_copy(sent, sent, ag_send.at[d]).wait()
        for j in range(PIECES):
            own_copy(d, j).wait()


def solution(mesh):
    n = mesh.shape["tp"]

    def step(x, w_gate, w_up, w_down):
        (rows, depth), width = x.shape, w_gate.shape[1]
        half = rows // n // 2
        fb, db = width // PIECES, depth // PIECES
        any_space = pl.BlockSpec(memory_space=pl.ANY)
        return pl.pallas_call(
            functools.partial(kernel, n),
            out_shape=jax.ShapeDtypeStruct((rows, depth), jnp.bfloat16),
            in_specs=[any_space] * 4,
            out_specs=any_space,
            scratch_shapes=[
                pltpu.VMEM((PIECES, depth, 2 * fb), jnp.bfloat16),
                pltpu.VMEM((PIECES, width, db), jnp.bfloat16),
                pltpu.VMEM((2, 2 * half, depth), jnp.bfloat16),
                pltpu.VMEM((2, 2 * half, width), jnp.bfloat16),
                pltpu.VMEM((2, n, PIECES, half, db), jnp.bfloat16),
                pltpu.SemaphoreType.DMA((2, PIECES)),
                pltpu.SemaphoreType.DMA((PIECES,)),
                pltpu.SemaphoreType.DMA((2, 2)),
                pltpu.SemaphoreType.DMA((2, n, PIECES)),
                pltpu.SemaphoreType.DMA((2, n, PIECES)),
                pltpu.SemaphoreType.DMA((2,)),
                pltpu.SemaphoreType.DMA((2,)),
                pltpu.SemaphoreType.DMA((2, PIECES)),
            ],
            cost_estimate=pl.CostEstimate(
                flops=6 * rows * depth * width,
                bytes_accessed=2 * (3 * depth * width + 4 * rows * depth),
                transcendentals=rows * width),
            compiler_params=pltpu.CompilerParams(
                collective_id=0, has_side_effects=True, vmem_limit_bytes=66_000_000),
        )(x, w_gate, w_up, w_down)

    return jax.shard_map(
        step,
        mesh=mesh,
        in_specs=(P("dp", None), P(None, "tp"), P(None, "tp"), P("tp", None)),
        out_specs=P("dp", None),
        check_vma=False,
    )
```

```python
import functools

import jax
import jax.numpy as jnp
from jax import lax
from jax.experimental import pallas as pl
from jax.experimental.pallas import tpu as pltpu
from jax.sharding import PartitionSpec as P

MESH = pl.DeviceIdType.MESH
PIECES = 7
AHEAD = 3
CW, CCW = 0, 1


def kernel(n, x_hbm, wg_hbm, wu_hbm, wd_hbm, buf, wgu, wd, xb, hid,
           wgu_sem, wd_sem, x_sem, rs_recv, ag_recv, rs_send, ag_send):
    me = lax.axis_index("tp")
    right, left = lax.rem(me + 1, n), lax.rem(me + n - 1, n)
    target = ({"tp": right}, {"tp": left})
    chunk = x_hbm.shape[0] // n
    half = chunk // 2
    fb = wgu.shape[2] // 2
    db = wd.shape[2]

    def rows(d, c):
        return pl.ds(pl.multiple_of(c * chunk + d * half, half), half)

    def rs_chunk(d, k):
        return lax.rem(me + (2 * n - 1 - k if d == CW else 1 + k), n)

    def ag_chunk(d, m):
        return lax.rem(me + (2 * n - m if d == CW else m), n)

    def cols(j):
        return pl.ds(pl.multiple_of(j * db, db), db)

    def x_copy(d, k):
        slot = lax.rem(k, 2)
        return pltpu.make_async_copy(
            x_hbm.at[rows(d, rs_chunk(d, k))], xb.at[slot, pl.ds(d * half, half)], x_sem.at[slot, d])

    def gu_copies(j):
        c = pl.ds(pl.multiple_of(j * fb, fb), fb)
        return (pltpu.make_async_copy(wg_hbm.at[:, c], wgu.at[j, :, pl.ds(0, fb)], wgu_sem.at[0, j]),
                pltpu.make_async_copy(wu_hbm.at[:, c], wgu.at[j, :, pl.ds(fb, fb)], wgu_sem.at[1, j]))

    def wd_copy(j):
        return pltpu.make_async_copy(wd_hbm.at[:, cols(j)], wd.at[j], wd_sem.at[j])

    def rs_copy(d, k, j):
        piece = buf.at[d, rs_chunk(d, k), j]
        return pltpu.make_async_remote_copy(
            src_ref=piece, dst_ref=piece,
            send_sem=rs_send.at[d, j], recv_sem=rs_recv.at[d, k + 1, j],
            device_id=target[d], device_id_type=MESH)

    def rs_wait(d, k, j):
        piece = buf.at[d, rs_chunk(d, k), j]
        pltpu.make_async_copy(piece, piece, rs_recv.at[d, k, j]).wait()

    def ag_copy(d, m, j):
        piece = buf.at[d, ag_chunk(d, m), j]
        return pltpu.make_async_remote_copy(
            src_ref=piece, dst_ref=piece,
            send_sem=ag_send.at[d], recv_sem=ag_recv.at[d, m + 1, j],
            device_id=target[d], device_id_type=MESH)

    def ag_wait(d, m, j):
        piece = buf.at[d, ag_chunk(d, m), j]
        pltpu.make_async_copy(piece, piece, ag_recv.at[d, m, j]).wait()

    def gate_up(slot, j):
        gu = jnp.dot(xb[slot], wgu[j], preferred_element_type=jnp.float32)
        h = jax.nn.gelu(gu[:, :fb]) * gu[:, fb:]
        hid[slot, :, pl.ds(pl.multiple_of(j * fb, fb), fb)] = h.astype(hid.dtype)

    def down(k, j, first):
        acc = jnp.dot(hid[lax.rem(k, 2)], wd[j], preferred_element_type=jnp.float32)
        for d in (CW, CCW):
            c = rs_chunk(d, k)
            part = acc[d * half:(d + 1) * half]
            if not first:
                rs_wait(d, k, j)
                part = part + buf[d, c, j].astype(jnp.float32)
            buf[d, c, j] = part.astype(buf.dtype)

    def start_gu(j):
        for c in gu_copies(j):
            c.start()

    def start_x(k):
        for d in (CW, CCW):
            x_copy(d, k).start()

    start_x(0)
    for j in range(AHEAD):
        start_gu(j)
    barrier = pltpu.get_barrier_semaphore()
    for d in (CW, CCW):
        pl.semaphore_signal(barrier, inc=1, device_id=target[d], device_id_type=MESH)

    for d in (CW, CCW):
        x_copy(d, 0).wait()

    def prologue(j, _):
        @pl.when(j < PIECES - AHEAD)
        def _():
            start_gu(j + AHEAD)

        @pl.when(j >= PIECES - AHEAD)
        def _():
            wd_copy(j - (PIECES - AHEAD)).start()

        for c in gu_copies(j):
            c.wait()
        gate_up(0, j)
        return 0

    lax.fori_loop(0, PIECES, prologue, 0)
    start_x(1)
    for j in range(AHEAD, PIECES):
        wd_copy(j).start()
    pl.semaphore_wait(barrier, 2)

    def sent(k, j):
        for d in (CW, CCW):
            rs_copy(d, k, j).wait_send()

    def step(k, first):
        def piece(j, _):
            if first:
                wd_copy(j).wait()
            down(k, j, first)
            if not first:
                sent(k - 1, j)
            for d in (CW, CCW):
                rs_copy(d, k, j).start()

            @pl.when(j == 0)
            def _():
                for d in (CW, CCW):
                    x_copy(d, k + 1).wait()

            gate_up(lax.rem(k + 1, 2), j)
            return 0

        lax.fori_loop(0, PIECES, piece, 0)

    step(0, True)

    def middle(k, _):
        start_x(k + 1)
        step(k, False)
        return 0

    lax.fori_loop(1, n - 1, middle, 0)

    def last(j, _):
        down(n - 1, j, False)
        sent(n - 2, j)
        for d in (CW, CCW):
            ag_copy(d, 0, j).start()
        return 0

    lax.fori_loop(0, PIECES, last, 0)

    def gather(m, forward):
        def piece(j, _):
            for d in (CW, CCW):
                ag_wait(d, m, j)
                if forward:
                    ag_copy(d, m, j).start()
            return 0

        lax.fori_loop(0, PIECES, piece, 0)

    def gather_forward(m, _):
        gather(m, True)
        return 0

    lax.fori_loop(1, n - 1, gather_forward, 0)
    gather(n - 1, False)

    for d in (CW, CCW):
        pieces = buf.at[d, pl.ds(0, n - 1)]
        pltpu.make_async_copy(pieces, pieces, ag_send.at[d]).wait()


def unpack(n, buf, y_hbm, sem):
    half, db = buf.shape[3:]

    def copy(d, c, j):
        rows = pl.ds(pl.multiple_of(c * 2 * half + d * half, half), half)
        return pltpu.make_async_copy(buf.at[d, c, j], y_hbm.at[rows, pl.ds(j * db, db)], sem)

    def start(c, _):
        for d in (CW, CCW):
            for j in range(PIECES):
                copy(d, c, j).start()
        return 0

    lax.fori_loop(0, n, start, 0)
    pltpu.make_async_copy(y_hbm, y_hbm, sem).wait()


def solution(mesh):
    n = mesh.shape["tp"]

    def step(x, w_gate, w_up, w_down):
        (rows, depth), width = x.shape, w_gate.shape[1]
        half = rows // n // 2
        fb, db = width // PIECES, depth // PIECES
        any_space = pl.BlockSpec(memory_space=pl.ANY)
        packed = pl.pallas_call(
            functools.partial(kernel, n),
            out_shape=pltpu.VMEM((2, n, PIECES, half, db), jnp.bfloat16),
            in_specs=[any_space] * 4,
            out_specs=pl.BlockSpec(memory_space=pltpu.VMEM),
            scratch_shapes=[
                pltpu.VMEM((PIECES, depth, 2 * fb), jnp.bfloat16),
                pltpu.VMEM((PIECES, width, db), jnp.bfloat16),
                pltpu.VMEM((2, 2 * half, depth), jnp.bfloat16),
                pltpu.VMEM((2, 2 * half, width), jnp.bfloat16),
                pltpu.SemaphoreType.DMA((2, PIECES)),
                pltpu.SemaphoreType.DMA((PIECES,)),
                pltpu.SemaphoreType.DMA((2, 2)),
                pltpu.SemaphoreType.DMA((2, n, PIECES)),
                pltpu.SemaphoreType.DMA((2, n, PIECES)),
                pltpu.SemaphoreType.DMA((2, PIECES)),
                pltpu.SemaphoreType.DMA((2,)),
            ],
            cost_estimate=pl.CostEstimate(
                flops=6 * rows * depth * width,
                bytes_accessed=2 * (3 * depth * width + rows * depth),
                transcendentals=rows * width),
            compiler_params=pltpu.CompilerParams(
                collective_id=0, has_side_effects=True, vmem_limit_bytes=50_000_000),
        )(x, w_gate, w_up, w_down)
        return pl.pallas_call(
            functools.partial(unpack, n),
            out_shape=jax.ShapeDtypeStruct((rows, depth), jnp.bfloat16),
            in_specs=[pl.BlockSpec(memory_space=pltpu.VMEM)],
            out_specs=any_space,
            scratch_shapes=[pltpu.SemaphoreType.DMA],
            compiler_params=pltpu.CompilerParams(vmem_limit_bytes=1_000_000),
        )(packed)

    return jax.shard_map(
        step,
        mesh=mesh,
        in_specs=(P("dp", None), P(None, "tp"), P(None, "tp"), P("tp", None)),
        out_specs=P("dp", None),
        check_vma=False,
    )
```

```python
import functools

import jax
import jax.numpy as jnp
from jax import lax
from jax.experimental import pallas as pl
from jax.experimental.pallas import tpu as pltpu
from jax.sharding import PartitionSpec as P

MESH = pl.DeviceIdType.MESH
PIECES = 7
AHEAD = 2
GROUPS = ((0, 4), (4, 3))
CW, CCW = 0, 1


def kernel(n, x_hbm, wg_hbm, wu_hbm, wd_hbm, buf, wgu, wd, xb, hid, lead,
           wgu_sem, wd_sem, x_sem, rs_recv, ag_recv, rs_send, ag_send):
    me = lax.axis_index("tp")
    right, left = lax.rem(me + 1, n), lax.rem(me + n - 1, n)
    target = ({"tp": right}, {"tp": left})
    chunk = x_hbm.shape[0] // n
    half = chunk // 2
    fb = wgu.shape[2] // 2
    db = wd.shape[2]

    def rows(d, c):
        return pl.ds(pl.multiple_of(c * chunk + d * half, half), half)

    def rs_chunk(d, k):
        return lax.rem(me + (2 * n - 1 - k if d == CW else 1 + k), n)

    def ag_chunk(d, m):
        return lax.rem(me + (2 * n - m if d == CW else m), n)

    def cols(j):
        return pl.ds(pl.multiple_of(j * db, db), db)

    def x_copy(d, k):
        slot = lax.rem(k, 2)
        return pltpu.make_async_copy(
            x_hbm.at[rows(d, rs_chunk(d, k))], xb.at[slot, pl.ds(d * half, half)], x_sem.at[slot, d])

    def gu_copies(j):
        c = pl.ds(pl.multiple_of(j * fb, fb), fb)
        return (pltpu.make_async_copy(wg_hbm.at[:, c], wgu.at[j, :, pl.ds(0, fb)], wgu_sem.at[0, j]),
                pltpu.make_async_copy(wu_hbm.at[:, c], wgu.at[j, :, pl.ds(fb, fb)], wgu_sem.at[1, j]))

    def wd_copy(j):
        return pltpu.make_async_copy(wd_hbm.at[:, cols(j)], wd.at[j], wd_sem.at[j])

    def rs_copy(d, k, j):
        piece = buf.at[d, rs_chunk(d, k), :, cols(j)]
        return pltpu.make_async_remote_copy(
            src_ref=piece, dst_ref=piece,
            send_sem=rs_send.at[d, j], recv_sem=rs_recv.at[d, k + 1, j],
            device_id=target[d], device_id_type=MESH)

    def rs_wait(d, k, j):
        piece = buf.at[d, rs_chunk(d, k), :, cols(j)]
        pltpu.make_async_copy(piece, piece, rs_recv.at[d, k, j]).wait()

    def ag_block(d, m, g):
        first, count = GROUPS[g]
        return buf.at[d, ag_chunk(d, m), :, pl.ds(first * db, count * db)]

    def ag_copy(d, m, g):
        block = ag_block(d, m, g)
        return pltpu.make_async_remote_copy(
            src_ref=block, dst_ref=block,
            send_sem=ag_send.at[d], recv_sem=ag_recv.at[d, m + 1, g],
            device_id=target[d], device_id_type=MESH)

    def ag_wait(d, m, g):
        block = ag_block(d, m, g)
        pltpu.make_async_copy(block, block, ag_recv.at[d, m, g]).wait()

    def gate_up(slot, j):
        gu = jnp.dot(xb[slot], wgu[j], preferred_element_type=jnp.float32)
        h = jax.nn.gelu(gu[:, :fb]) * gu[:, fb:]
        hid[slot, :, pl.ds(pl.multiple_of(j * fb, fb), fb)] = h.astype(hid.dtype)

    def put(acc, k, j, first):
        for d in (CW, CCW):
            c = rs_chunk(d, k)
            part = acc[d * half:(d + 1) * half]
            if not first:
                rs_wait(d, k, j)
                part = part + buf[d, c, :, cols(j)].astype(jnp.float32)
            buf[d, c, :, cols(j)] = part.astype(buf.dtype)

    def down(k, j, first):
        put(jnp.dot(hid[lax.rem(k, 2)], wd[j], preferred_element_type=jnp.float32), k, j, first)

    def start_gu(j):
        for c in gu_copies(j):
            c.start()

    def start_x(k):
        for d in (CW, CCW):
            x_copy(d, k).start()

    start_x(0)
    start_gu(0)
    wd_copy(0).start()
    for j in range(1, AHEAD):
        start_gu(j)
    barrier = pltpu.get_barrier_semaphore()
    for d in (CW, CCW):
        pl.semaphore_signal(barrier, inc=1, device_id=target[d], device_id_type=MESH)

    for d in (CW, CCW):
        x_copy(d, 0).wait()

    wd_copy(0).wait()
    lead[...] = jnp.zeros_like(lead)

    def prologue(j, _):
        @pl.when(j < PIECES - AHEAD)
        def _():
            start_gu(j + AHEAD)

        for c in gu_copies(j):
            c.wait()

        @pl.when(j == PIECES - 1)
        def _():
            start_x(1)
            for i in range(1, PIECES):
                wd_copy(i).start()

        gate_up(0, j)
        f = pl.ds(pl.multiple_of(j * fb, fb), fb)
        lead[...] += jnp.dot(hid[0, :, f], wd[0, f], preferred_element_type=jnp.float32)
        return 0

    lax.fori_loop(0, PIECES, prologue, 0)
    pl.semaphore_wait(barrier, 2)

    def sent(k, j):
        for d in (CW, CCW):
            rs_copy(d, k, j).wait_send()

    def send(k, j):
        for d in (CW, CCW):
            rs_copy(d, k, j).start()

    put(lead[...], 0, 0, True)
    send(0, 0)
    for d in (CW, CCW):
        x_copy(d, 1).wait()
    gate_up(1, 0)

    def first(j, _):
        wd_copy(j).wait()
        down(0, j, True)
        send(0, j)
        gate_up(1, j)
        return 0

    lax.fori_loop(1, PIECES, first, 0)

    def step(k):
        def piece(j, _):
            down(k, j, False)
            sent(k - 1, j)
            send(k, j)

            @pl.when(j == 0)
            def _():
                for d in (CW, CCW):
                    x_copy(d, k + 1).wait()

            gate_up(lax.rem(k + 1, 2), j)
            return 0

        lax.fori_loop(0, PIECES, piece, 0)

    def middle(k, _):
        start_x(k + 1)
        step(k)
        return 0

    lax.fori_loop(1, n - 1, middle, 0)

    for g, (start, count) in enumerate(GROUPS):
        def last(j, _):
            down(n - 1, j, False)
            sent(n - 2, j)
            return 0

        lax.fori_loop(start, start + count, last, 0)
        for d in (CW, CCW):
            ag_copy(d, 0, g).start()

    def gather(m, forward):
        for g in range(len(GROUPS)):
            for d in (CW, CCW):
                ag_wait(d, m, g)
                if forward:
                    ag_copy(d, m, g).start()

    def gather_forward(m, _):
        gather(m, True)
        return 0

    lax.fori_loop(1, n - 1, gather_forward, 0)
    gather(n - 1, False)

    for d in (CW, CCW):
        pieces = buf.at[d, pl.ds(0, n - 1)]
        pltpu.make_async_copy(pieces, pieces, ag_send.at[d]).wait()


def unpack(n, buf, y_hbm, sem):
    half = buf.shape[2]
    for c in range(n):
        for d in (CW, CCW):
            pltpu.make_async_copy(buf.at[d, c], y_hbm.at[pl.ds((2 * c + d) * half, half)], sem).start()
    pltpu.make_async_copy(y_hbm, y_hbm, sem).wait()


def solution(mesh):
    n = mesh.shape["tp"]

    def step(x, w_gate, w_up, w_down):
        (rows, depth), width = x.shape, w_gate.shape[1]
        half = rows // n // 2
        fb, db = width // PIECES, depth // PIECES
        any_space = pl.BlockSpec(memory_space=pl.ANY)
        packed = pl.pallas_call(
            functools.partial(kernel, n),
            out_shape=pltpu.VMEM((2, n, half, depth), jnp.bfloat16),
            in_specs=[any_space] * 4,
            out_specs=pl.BlockSpec(memory_space=pltpu.VMEM),
            scratch_shapes=[
                pltpu.VMEM((PIECES, depth, 2 * fb), jnp.bfloat16),
                pltpu.VMEM((PIECES, width, db), jnp.bfloat16),
                pltpu.VMEM((2, 2 * half, depth), jnp.bfloat16),
                pltpu.VMEM((2, 2 * half, width), jnp.bfloat16),
                pltpu.VMEM((2 * half, db), jnp.float32),
                pltpu.SemaphoreType.DMA((2, PIECES)),
                pltpu.SemaphoreType.DMA((PIECES,)),
                pltpu.SemaphoreType.DMA((2, 2)),
                pltpu.SemaphoreType.DMA((2, n, PIECES)),
                pltpu.SemaphoreType.DMA((2, n, len(GROUPS))),
                pltpu.SemaphoreType.DMA((2, PIECES)),
                pltpu.SemaphoreType.DMA((2,)),
            ],
            cost_estimate=pl.CostEstimate(
                flops=6 * rows * depth * width,
                bytes_accessed=2 * (3 * depth * width + rows * depth),
                transcendentals=rows * width),
            compiler_params=pltpu.CompilerParams(
                collective_id=0, has_side_effects=True, vmem_limit_bytes=50_000_000),
        )(x, w_gate, w_up, w_down)
        return pl.pallas_call(
            functools.partial(unpack, n),
            out_shape=jax.ShapeDtypeStruct((rows, depth), jnp.bfloat16),
            in_specs=[pl.BlockSpec(memory_space=pltpu.VMEM)],
            out_specs=any_space,
            scratch_shapes=[pltpu.SemaphoreType.DMA],
            compiler_params=pltpu.CompilerParams(vmem_limit_bytes=1_000_000),
        )(packed)

    return jax.shard_map(
        step,
        mesh=mesh,
        in_specs=(P("dp", None), P(None, "tp"), P(None, "tp"), P("tp", None)),
        out_specs=P("dp", None),
        check_vma=False,
    )
```

```python
import functools

import jax
import jax.numpy as jnp
from jax import lax
from jax.experimental import pallas as pl
from jax.experimental.pallas import tpu as pltpu
from jax.sharding import PartitionSpec as P

MESH = pl.DeviceIdType.MESH
PIECES = 7
AHEAD = 2
SHARED = 2
GROUPS = ((0, 4), (4, 3))
CW, CCW = 0, 1


def kernel(n, x_hbm, wg_hbm, wu_hbm, wd_hbm, buf, wgu, wd, xb, hid, lead,
           wgu_sem, wd_sem, x_sem, rs_recv, ag_recv, rs_send, ag_send, pair_send):
    me = lax.axis_index("tp")
    right, left = lax.rem(me + 1, n), lax.rem(me + n - 1, n)
    target = ({"tp": right}, {"tp": left})
    group = lax.axis_index("dp")
    side = lax.rem(group, 2)
    pair = {"dp": group + 1 - 2 * side}
    chunk = x_hbm.shape[0] // n
    half = chunk // 2
    fb = wgu.shape[2] // 2
    db = wd.shape[2]

    def rows(d, c):
        return pl.ds(pl.multiple_of(c * chunk + d * half, half), half)

    def rs_chunk(d, k):
        return lax.rem(me + (2 * n - 1 - k if d == CW else 1 + k), n)

    def ag_chunk(d, m):
        return lax.rem(me + (2 * n - m if d == CW else m), n)

    def cols(j):
        return pl.ds(pl.multiple_of(j * db, db), db)

    def x_copy(d, k):
        slot = lax.rem(k, 2)
        return pltpu.make_async_copy(
            x_hbm.at[rows(d, rs_chunk(d, k))], xb.at[slot, pl.ds(d * half, half)], x_sem.at[slot, d])

    def gu_copies(j):
        c = pl.ds(pl.multiple_of(j * fb, fb), fb)
        return (pltpu.make_async_copy(wg_hbm.at[:, c], wgu.at[j, :, pl.ds(0, fb)], wgu_sem.at[0, j]),
                pltpu.make_async_copy(wu_hbm.at[:, c], wgu.at[j, :, pl.ds(fb, fb)], wgu_sem.at[1, j]))

    def half_block(j):
        return wgu.at[j, :, pl.ds(pl.multiple_of(side * fb, fb), fb)]

    def start_half(j):
        for i in (0, 1):
            @pl.when(side == i)
            def _(i=i):
                gu_copies(j)[i].start()

    def wait_half(j, i):
        pltpu.make_async_copy(half_block(j), half_block(j), wgu_sem.at[i, j]).wait()

    def pair_copy(j):
        return pltpu.make_async_remote_copy(
            src_ref=half_block(j), dst_ref=half_block(j),
            send_sem=pair_send.at[j - (PIECES - SHARED)], recv_sem=wgu_sem.at[side, j],
            device_id=pair, device_id_type=MESH)

    def wd_copy(j):
        return pltpu.make_async_copy(wd_hbm.at[:, cols(j)], wd.at[j], wd_sem.at[j])

    def rs_copy(d, k, j):
        piece = buf.at[d, rs_chunk(d, k), :, cols(j)]
        return pltpu.make_async_remote_copy(
            src_ref=piece, dst_ref=piece,
            send_sem=rs_send.at[d, j], recv_sem=rs_recv.at[d, k + 1, j],
            device_id=target[d], device_id_type=MESH)

    def rs_wait(d, k, j):
        piece = buf.at[d, rs_chunk(d, k), :, cols(j)]
        pltpu.make_async_copy(piece, piece, rs_recv.at[d, k, j]).wait()

    def ag_block(d, m, g):
        first, count = GROUPS[g]
        return buf.at[d, ag_chunk(d, m), :, pl.ds(first * db, count * db)]

    def ag_copy(d, m, g):
        block = ag_block(d, m, g)
        return pltpu.make_async_remote_copy(
            src_ref=block, dst_ref=block,
            send_sem=ag_send.at[d], recv_sem=ag_recv.at[d, m + 1, g],
            device_id=target[d], device_id_type=MESH)

    def ag_wait(d, m, g):
        block = ag_block(d, m, g)
        pltpu.make_async_copy(block, block, ag_recv.at[d, m, g]).wait()

    def gate_up(slot, j):
        gu = jnp.dot(xb[slot], wgu[j], preferred_element_type=jnp.float32)
        h = jax.nn.gelu(gu[:, :fb]) * gu[:, fb:]
        hid[slot, :, pl.ds(pl.multiple_of(j * fb, fb), fb)] = h.astype(hid.dtype)

    def put(acc, k, j, first):
        for d in (CW, CCW):
            c = rs_chunk(d, k)
            part = acc[d * half:(d + 1) * half]
            if not first:
                rs_wait(d, k, j)
                part = part + buf[d, c, :, cols(j)].astype(jnp.float32)
            buf[d, c, :, cols(j)] = part.astype(buf.dtype)

    def down(k, j, first):
        put(jnp.dot(hid[lax.rem(k, 2)], wd[j], preferred_element_type=jnp.float32), k, j, first)

    def start_gu(j):
        for c in gu_copies(j):
            c.start()

    def start_x(k):
        for d in (CW, CCW):
            x_copy(d, k).start()

    shared = range(PIECES - SHARED, PIECES)
    for j in shared:
        start_half(j)
    start_x(0)
    start_gu(0)
    wd_copy(0).start()
    for j in range(1, AHEAD):
        start_gu(j)
    barrier = pltpu.get_barrier_semaphore()
    for d in (CW, CCW):
        pl.semaphore_signal(barrier, inc=1, device_id=target[d], device_id_type=MESH)
    pl.semaphore_signal(barrier, inc=1, device_id=pair, device_id_type=MESH)
    pl.semaphore_wait(barrier, 3)
    for j in shared:
        wait_half(j, side)
        pair_copy(j).start()

    for d in (CW, CCW):
        x_copy(d, 0).wait()

    wd_copy(0).wait()
    lead[...] = jnp.zeros_like(lead)

    def prologue(j, _):
        @pl.when(j < PIECES - SHARED - AHEAD)
        def _():
            start_gu(j + AHEAD)

        @pl.when(j < PIECES - SHARED)
        def _():
            for c in gu_copies(j):
                c.wait()

        @pl.when(j >= PIECES - SHARED)
        def _():
            wait_half(j, 1 - side)

        @pl.when(j == PIECES - SHARED)
        def _():
            start_x(1)
            for i in range(1, PIECES):
                wd_copy(i).start()

        gate_up(0, j)
        f = pl.ds(pl.multiple_of(j * fb, fb), fb)
        lead[...] += jnp.dot(hid[0, :, f], wd[0, f], preferred_element_type=jnp.float32)
        return 0

    lax.fori_loop(0, PIECES, prologue, 0)

    def sent(k, j):
        for d in (CW, CCW):
            rs_copy(d, k, j).wait_send()

    def send(k, j):
        for d in (CW, CCW):
            rs_copy(d, k, j).start()

    put(lead[...], 0, 0, True)
    send(0, 0)
    for d in (CW, CCW):
        x_copy(d, 1).wait()
    gate_up(1, 0)

    def first(j, _):
        wd_copy(j).wait()
        down(0, j, True)
        send(0, j)
        gate_up(1, j)
        return 0

    lax.fori_loop(1, PIECES, first, 0)

    def step(k):
        def piece(j, _):
            down(k, j, False)
            sent(k - 1, j)
            send(k, j)

            @pl.when(j == 0)
            def _():
                for d in (CW, CCW):
                    x_copy(d, k + 1).wait()

            gate_up(lax.rem(k + 1, 2), j)
            return 0

        lax.fori_loop(0, PIECES, piece, 0)

    def middle(k, _):
        start_x(k + 1)
        step(k)
        return 0

    lax.fori_loop(1, n - 1, middle, 0)

    for g, (start, count) in enumerate(GROUPS):
        def last(j, _):
            down(n - 1, j, False)
            sent(n - 2, j)
            return 0

        lax.fori_loop(start, start + count, last, 0)
        for d in (CW, CCW):
            ag_copy(d, 0, g).start()

    def gather(m, forward):
        for g in range(len(GROUPS)):
            for d in (CW, CCW):
                ag_wait(d, m, g)
                if forward:
                    ag_copy(d, m, g).start()

    def gather_forward(m, _):
        gather(m, True)
        return 0

    lax.fori_loop(1, n - 1, gather_forward, 0)
    gather(n - 1, False)

    for j in shared:
        pair_copy(j).wait_send()
    for d in (CW, CCW):
        pieces = buf.at[d, pl.ds(0, n - 1)]
        pltpu.make_async_copy(pieces, pieces, ag_send.at[d]).wait()


def unpack(n, buf, y_hbm, sem):
    half = buf.shape[2]
    for c in range(n):
        for d in (CW, CCW):
            pltpu.make_async_copy(buf.at[d, c], y_hbm.at[pl.ds((2 * c + d) * half, half)], sem).start()
    pltpu.make_async_copy(y_hbm, y_hbm, sem).wait()


def solution(mesh):
    n = mesh.shape["tp"]

    def step(x, w_gate, w_up, w_down):
        (rows, depth), width = x.shape, w_gate.shape[1]
        half = rows // n // 2
        fb, db = width // PIECES, depth // PIECES
        any_space = pl.BlockSpec(memory_space=pl.ANY)
        packed = pl.pallas_call(
            functools.partial(kernel, n),
            out_shape=pltpu.VMEM((2, n, half, depth), jnp.bfloat16),
            in_specs=[any_space] * 4,
            out_specs=pl.BlockSpec(memory_space=pltpu.VMEM),
            scratch_shapes=[
                pltpu.VMEM((PIECES, depth, 2 * fb), jnp.bfloat16),
                pltpu.VMEM((PIECES, width, db), jnp.bfloat16),
                pltpu.VMEM((2, 2 * half, depth), jnp.bfloat16),
                pltpu.VMEM((2, 2 * half, width), jnp.bfloat16),
                pltpu.VMEM((2 * half, db), jnp.float32),
                pltpu.SemaphoreType.DMA((2, PIECES)),
                pltpu.SemaphoreType.DMA((PIECES,)),
                pltpu.SemaphoreType.DMA((2, 2)),
                pltpu.SemaphoreType.DMA((2, n, PIECES)),
                pltpu.SemaphoreType.DMA((2, n, len(GROUPS))),
                pltpu.SemaphoreType.DMA((2, PIECES)),
                pltpu.SemaphoreType.DMA((2,)),
                pltpu.SemaphoreType.DMA((SHARED,)),
            ],
            cost_estimate=pl.CostEstimate(
                flops=6 * rows * depth * width,
                bytes_accessed=2 * (3 * depth * width + rows * depth),
                transcendentals=rows * width),
            compiler_params=pltpu.CompilerParams(
                collective_id=0, has_side_effects=True, vmem_limit_bytes=50_000_000),
        )(x, w_gate, w_up, w_down)
        return pl.pallas_call(
            functools.partial(unpack, n),
            out_shape=jax.ShapeDtypeStruct((rows, depth), jnp.bfloat16),
            in_specs=[pl.BlockSpec(memory_space=pltpu.VMEM)],
            out_specs=any_space,
            scratch_shapes=[pltpu.SemaphoreType.DMA],
            compiler_params=pltpu.CompilerParams(vmem_limit_bytes=1_000_000),
        )(packed)

    return jax.shard_map(
        step,
        mesh=mesh,
        in_specs=(P("dp", None), P(None, "tp"), P(None, "tp"), P("tp", None)),
        out_specs=P("dp", None),
        check_vma=False,
    )
```

```python
import functools

import jax
import jax.numpy as jnp
from jax import lax
from jax.experimental import pallas as pl
from jax.experimental.pallas import tpu as pltpu
from jax.sharding import PartitionSpec as P

MESH = pl.DeviceIdType.MESH
PIECES = 7
AHEAD = 2
GROUPS = ((0, 4), (4, 3))
CW, CCW = 0, 1


def kernel(n, x_hbm, wg_hbm, wu_hbm, wd_hbm, buf, wgu, wd, xb, hid,
           wgu_sem, wd_sem, x_sem, x0_sem, rs_recv, ag_recv, rs_send, ag_send):
    me = lax.axis_index("tp")
    right, left = lax.rem(me + 1, n), lax.rem(me + n - 1, n)
    target = ({"tp": right}, {"tp": left})
    chunk = x_hbm.shape[0] // n
    half = chunk // 2
    quarter = half // 2
    fb = wgu.shape[2] // 2
    db = wd.shape[2]

    def rows(d, c):
        return pl.ds(pl.multiple_of(c * chunk + d * half, half), half)

    def rs_chunk(d, k):
        return lax.rem(me + (2 * n - 1 - k if d == CW else 1 + k), n)

    def ag_chunk(d, m):
        return lax.rem(me + (2 * n - m if d == CW else m), n)

    def cols(j):
        return pl.ds(pl.multiple_of(j * db, db), db)

    def x_copy(d, k):
        slot = lax.rem(k, 2)
        return pltpu.make_async_copy(
            x_hbm.at[rows(d, rs_chunk(d, k))], xb.at[slot, pl.ds(d * half, half)], x_sem.at[slot, d])

    def x0_copy(d, r):
        start = rs_chunk(d, 0) * chunk + d * half + r * quarter
        return pltpu.make_async_copy(
            x_hbm.at[pl.ds(pl.multiple_of(start, quarter), quarter)],
            xb.at[0, pl.ds((2 * r + d) * quarter, quarter)], x0_sem.at[r, d])

    def gu_copies(j):
        c = pl.ds(pl.multiple_of(j * fb, fb), fb)
        return (pltpu.make_async_copy(wg_hbm.at[:, c], wgu.at[j, :, pl.ds(0, fb)], wgu_sem.at[0, j]),
                pltpu.make_async_copy(wu_hbm.at[:, c], wgu.at[j, :, pl.ds(fb, fb)], wgu_sem.at[1, j]))

    def wd_copy(j):
        return pltpu.make_async_copy(wd_hbm.at[:, cols(j)], wd.at[j], wd_sem.at[j])

    def rs_copy(d, k, j):
        piece = buf.at[d, rs_chunk(d, k), :, cols(j)]
        return pltpu.make_async_remote_copy(
            src_ref=piece, dst_ref=piece,
            send_sem=rs_send.at[d, j], recv_sem=rs_recv.at[d, k + 1, j],
            device_id=target[d], device_id_type=MESH)

    def rs_wait(d, k, j):
        piece = buf.at[d, rs_chunk(d, k), :, cols(j)]
        pltpu.make_async_copy(piece, piece, rs_recv.at[d, k, j]).wait()

    def ag_block(d, m, g):
        first, count = GROUPS[g]
        return buf.at[d, ag_chunk(d, m), :, pl.ds(first * db, count * db)]

    def ag_copy(d, m, g):
        block = ag_block(d, m, g)
        return pltpu.make_async_remote_copy(
            src_ref=block, dst_ref=block,
            send_sem=ag_send.at[d], recv_sem=ag_recv.at[d, m + 1, g],
            device_id=target[d], device_id_type=MESH)

    def ag_wait(d, m, g):
        block = ag_block(d, m, g)
        pltpu.make_async_copy(block, block, ag_recv.at[d, m, g]).wait()

    def gate_up(slot, j, rows=slice(None)):
        gu = jnp.dot(xb[slot, rows], wgu[j], preferred_element_type=jnp.float32)
        h = jax.nn.gelu(gu[:, :fb]) * gu[:, fb:]
        hid[slot, rows, pl.ds(pl.multiple_of(j * fb, fb), fb)] = h.astype(hid.dtype)

    def down(k, j):
        acc = jnp.dot(hid[lax.rem(k, 2)], wd[j], preferred_element_type=jnp.float32)
        for d in (CW, CCW):
            c = rs_chunk(d, k)
            rs_wait(d, k, j)
            total = acc[d * half:(d + 1) * half] + buf[d, c, :, cols(j)].astype(jnp.float32)
            buf[d, c, :, cols(j)] = total.astype(buf.dtype)

    def start_gu(j):
        for c in gu_copies(j):
            c.start()

    def start_x(k):
        for d in (CW, CCW):
            x_copy(d, k).start()

    def start_x0(r):
        for d in (CW, CCW):
            x0_copy(d, r).start()

    def wait_x0(r):
        for d in (CW, CCW):
            x0_copy(d, r).wait()

    start_x0(0)
    for j in range(AHEAD):
        start_gu(j)
    barrier = pltpu.get_barrier_semaphore()
    for d in (CW, CCW):
        pl.semaphore_signal(barrier, inc=1, device_id=target[d], device_id_type=MESH)

    part = [slice(r * half, (r + 1) * half) for r in (0, 1)]
    wait_x0(0)

    def prologue(j, _):
        @pl.when(j < PIECES - AHEAD)
        def _():
            start_gu(j + AHEAD)

        @pl.when(j >= PIECES - AHEAD)
        def _():
            wd_copy(j - (PIECES - AHEAD)).start()

        @pl.when(j == PIECES // 2)
        def _():
            start_x0(1)

        for c in gu_copies(j):
            c.wait()
        gate_up(0, j, part[0])
        return 0

    lax.fori_loop(0, PIECES, prologue, 0)
    for j in range(AHEAD, PIECES):
        wd_copy(j).start()
    start_x(1)
    pl.semaphore_wait(barrier, 2)
    wait_x0(1)

    def send(k, j):
        for d in (CW, CCW):
            rs_copy(d, k, j).start()

    def sent(k, j):
        for d in (CW, CCW):
            rs_copy(d, k, j).wait_send()

    def send_part(r, j):
        acc = jnp.dot(hid[0, part[r]], wd[j], preferred_element_type=jnp.float32)
        for d in (CW, CCW):
            piece = buf.at[d, rs_chunk(d, 0), pl.ds(r * quarter, quarter), cols(j)]
            piece[...] = acc[d * quarter:(d + 1) * quarter].astype(buf.dtype)
            pltpu.make_async_remote_copy(
                src_ref=piece, dst_ref=piece,
                send_sem=rs_send.at[d, j], recv_sem=rs_recv.at[d, 1, j],
                device_id=target[d], device_id_type=MESH).start()

    def first(j, _):
        wd_copy(j).wait()
        send_part(0, j)
        gate_up(0, j, part[1])
        return 0

    def second(j, _):
        send_part(1, j)
        gate_up(1, j)
        return 0

    lax.fori_loop(0, PIECES, first, 0)
    for d in (CW, CCW):
        x_copy(d, 1).wait()
    lax.fori_loop(0, PIECES, second, 0)

    def step(k):
        def piece(j, _):
            down(k, j)
            sent(k - 1, j)
            send(k, j)

            @pl.when(j == 0)
            def _():
                for d in (CW, CCW):
                    x_copy(d, k + 1).wait()

            gate_up(lax.rem(k + 1, 2), j)
            return 0

        lax.fori_loop(0, PIECES, piece, 0)

    def middle(k, _):
        start_x(k + 1)
        step(k)
        return 0

    lax.fori_loop(1, n - 1, middle, 0)

    for g, (start, count) in enumerate(GROUPS):
        def last(j, _):
            down(n - 1, j)
            sent(n - 2, j)
            return 0

        lax.fori_loop(start, start + count, last, 0)
        for d in (CW, CCW):
            ag_copy(d, 0, g).start()

    def gather(m, forward):
        for g in range(len(GROUPS)):
            for d in (CW, CCW):
                ag_wait(d, m, g)
                if forward:
                    ag_copy(d, m, g).start()

    def gather_forward(m, _):
        gather(m, True)
        return 0

    lax.fori_loop(1, n - 1, gather_forward, 0)
    gather(n - 1, False)

    for d in (CW, CCW):
        pieces = buf.at[d, pl.ds(0, n - 1)]
        pltpu.make_async_copy(pieces, pieces, ag_send.at[d]).wait()


def unpack(n, buf, y_hbm, sem):
    half = buf.shape[2]
    for c in range(n):
        for d in (CW, CCW):
            pltpu.make_async_copy(buf.at[d, c], y_hbm.at[pl.ds((2 * c + d) * half, half)], sem).start()
    pltpu.make_async_copy(y_hbm, y_hbm, sem).wait()


def solution(mesh):
    n = mesh.shape["tp"]

    def step(x, w_gate, w_up, w_down):
        (rows, depth), width = x.shape, w_gate.shape[1]
        half = rows // n // 2
        fb, db = width // PIECES, depth // PIECES
        any_space = pl.BlockSpec(memory_space=pl.ANY)
        packed = pl.pallas_call(
            functools.partial(kernel, n),
            out_shape=pltpu.VMEM((2, n, half, depth), jnp.bfloat16),
            in_specs=[any_space] * 4,
            out_specs=pl.BlockSpec(memory_space=pltpu.VMEM),
            scratch_shapes=[
                pltpu.VMEM((PIECES, depth, 2 * fb), jnp.bfloat16),
                pltpu.VMEM((PIECES, width, db), jnp.bfloat16),
                pltpu.VMEM((2, 2 * half, depth), jnp.bfloat16),
                pltpu.VMEM((2, 2 * half, width), jnp.bfloat16),
                pltpu.SemaphoreType.DMA((2, PIECES)),
                pltpu.SemaphoreType.DMA((PIECES,)),
                pltpu.SemaphoreType.DMA((2, 2)),
                pltpu.SemaphoreType.DMA((2, 2)),
                pltpu.SemaphoreType.DMA((2, n, PIECES)),
                pltpu.SemaphoreType.DMA((2, n, len(GROUPS))),
                pltpu.SemaphoreType.DMA((2, PIECES)),
                pltpu.SemaphoreType.DMA((2,)),
            ],
            cost_estimate=pl.CostEstimate(
                flops=6 * rows * depth * width,
                bytes_accessed=2 * (3 * depth * width + rows * depth),
                transcendentals=rows * width),
            compiler_params=pltpu.CompilerParams(
                collective_id=0, has_side_effects=True, vmem_limit_bytes=50_000_000),
        )(x, w_gate, w_up, w_down)
        return pl.pallas_call(
            functools.partial(unpack, n),
            out_shape=jax.ShapeDtypeStruct((rows, depth), jnp.bfloat16),
            in_specs=[pl.BlockSpec(memory_space=pltpu.VMEM)],
            out_specs=any_space,
            scratch_shapes=[pltpu.SemaphoreType.DMA],
            compiler_params=pltpu.CompilerParams(vmem_limit_bytes=1_000_000),
        )(packed)

    return jax.shard_map(
        step,
        mesh=mesh,
        in_specs=(P("dp", None), P(None, "tp"), P(None, "tp"), P("tp", None)),
        out_specs=P("dp", None),
        check_vma=False,
    )
```

```python
import functools

import jax
import jax.numpy as jnp
from jax import lax
from jax.experimental import pallas as pl
from jax.experimental.pallas import tpu as pltpu
from jax.sharding import PartitionSpec as P

MESH = pl.DeviceIdType.MESH
PIECES = 7
AHEAD = 2
GROUPS = ((0, 4), (4, 3))
CW, CCW = 0, 1


def kernel(n, x_hbm, wg_hbm, wu_hbm, wd_hbm, buf, wgu, wd, xb, hid,
           wgu_sem, wd_sem, x_sem, x0_sem, rs_recv, ag_recv, rs_send, ag_send):
    me = lax.axis_index("tp")
    right, left = lax.rem(me + 1, n), lax.rem(me + n - 1, n)
    target = ({"tp": right}, {"tp": left})
    chunk = x_hbm.shape[0] // n
    half = chunk // 2
    quarter = half // 2
    fb = wgu.shape[2] // 2
    db = wd.shape[2]

    def rows(d, c):
        return pl.ds(pl.multiple_of(c * chunk + d * half, half), half)

    def rs_chunk(d, k):
        return lax.rem(me + (2 * n - 1 - k if d == CW else 1 + k), n)

    def ag_chunk(d, m):
        return lax.rem(me + (2 * n - m if d == CW else m), n)

    def cols(j):
        return pl.ds(pl.multiple_of(j * db, db), db)

    def x_copy(d, k):
        slot = lax.rem(k, 2)
        return pltpu.make_async_copy(
            x_hbm.at[rows(d, rs_chunk(d, k))], xb.at[slot, pl.ds(d * half, half)], x_sem.at[slot, d])

    def x0_copy(d, r):
        start = rs_chunk(d, 0) * chunk + d * half + r * quarter
        return pltpu.make_async_copy(
            x_hbm.at[pl.ds(pl.multiple_of(start, quarter), quarter)],
            xb.at[0, pl.ds((2 * r + d) * quarter, quarter)], x0_sem.at[r, d])

    def gu_copies(j):
        c = pl.ds(pl.multiple_of(j * fb, fb), fb)
        return (pltpu.make_async_copy(wg_hbm.at[:, c], wgu.at[j, :, pl.ds(0, fb)], wgu_sem.at[0, j]),
                pltpu.make_async_copy(wu_hbm.at[:, c], wgu.at[j, :, pl.ds(fb, fb)], wgu_sem.at[1, j]))

    def wd_copy(j):
        return pltpu.make_async_copy(wd_hbm.at[:, cols(j)], wd.at[j], wd_sem.at[j])

    def rs_copy(d, k, j):
        piece = buf.at[d, rs_chunk(d, k), :, cols(j)]
        return pltpu.make_async_remote_copy(
            src_ref=piece, dst_ref=piece,
            send_sem=rs_send.at[d, j], recv_sem=rs_recv.at[d, k + 1, j],
            device_id=target[d], device_id_type=MESH)

    def rs_wait(d, k, j):
        piece = buf.at[d, rs_chunk(d, k), :, cols(j)]
        pltpu.make_async_copy(piece, piece, rs_recv.at[d, k, j]).wait()

    def ag_block(d, m, g):
        first, count = GROUPS[g]
        return buf.at[d, ag_chunk(d, m), :, pl.ds(first * db, count * db)]

    def ag_copy(d, m, g):
        block = ag_block(d, m, g)
        return pltpu.make_async_remote_copy(
            src_ref=block, dst_ref=block,
            send_sem=ag_send.at[d], recv_sem=ag_recv.at[d, m + 1, g],
            device_id=target[d], device_id_type=MESH)

    def ag_wait(d, m, g):
        block = ag_block(d, m, g)
        pltpu.make_async_copy(block, block, ag_recv.at[d, m, g]).wait()

    def gate_up(slot, j, rows=slice(None)):
        gu = jnp.dot(xb[slot, rows], wgu[j], preferred_element_type=jnp.float32)
        h = jax.nn.gelu(gu[:, :fb]) * gu[:, fb:]
        hid[slot, rows, pl.ds(pl.multiple_of(j * fb, fb), fb)] = h.astype(hid.dtype)

    def down(k, j):
        acc = jnp.dot(hid[lax.rem(k, 2)], wd[j], preferred_element_type=jnp.float32)
        for d in (CW, CCW):
            c = rs_chunk(d, k)
            rs_wait(d, k, j)
            total = acc[d * half:(d + 1) * half] + buf[d, c, :, cols(j)].astype(jnp.float32)
            buf[d, c, :, cols(j)] = total.astype(buf.dtype)

    def start_gu(j):
        for c in gu_copies(j):
            c.start()

    def start_x(k):
        for d in (CW, CCW):
            x_copy(d, k).start()

    def start_x0(r):
        for d in (CW, CCW):
            x0_copy(d, r).start()

    def wait_x0(r):
        for d in (CW, CCW):
            x0_copy(d, r).wait()

    start_x0(0)
    for j in range(AHEAD):
        start_gu(j)
    barrier = pltpu.get_barrier_semaphore()
    for d in (CW, CCW):
        pl.semaphore_signal(barrier, inc=1, device_id=target[d], device_id_type=MESH)

    part = [slice(r * half, (r + 1) * half) for r in (0, 1)]
    wait_x0(0)

    def prologue(j, _):
        @pl.when(j < PIECES - AHEAD)
        def _():
            start_gu(j + AHEAD)

        @pl.when(j == PIECES - AHEAD)
        def _():
            wd_copy(0).start()

        for c in gu_copies(j):
            c.wait()

        @pl.when(j == PIECES - 1)
        def _():
            start_x0(1)
            for i in range(1, PIECES):
                wd_copy(i).start()
            start_x(1)

        gate_up(0, j, part[0])
        return 0

    lax.fori_loop(0, PIECES, prologue, 0)
    pl.semaphore_wait(barrier, 2)

    def send(k, j):
        for d in (CW, CCW):
            rs_copy(d, k, j).start()

    def sent(k, j):
        for d in (CW, CCW):
            rs_copy(d, k, j).wait_send()

    def send_part(r, j):
        acc = jnp.dot(hid[0, part[r]], wd[j], preferred_element_type=jnp.float32)
        for d in (CW, CCW):
            piece = buf.at[d, rs_chunk(d, 0), pl.ds(r * quarter, quarter), cols(j)]
            piece[...] = acc[d * quarter:(d + 1) * quarter].astype(buf.dtype)
            pltpu.make_async_remote_copy(
                src_ref=piece, dst_ref=piece,
                send_sem=rs_send.at[d, j], recv_sem=rs_recv.at[d, 1, j],
                device_id=target[d], device_id_type=MESH).start()

    def first(j, _):
        wd_copy(j).wait()
        send_part(0, j)

        @pl.when(j == 0)
        def _():
            wait_x0(1)

        gate_up(0, j, part[1])
        return 0

    def second(j, _):
        send_part(1, j)
        gate_up(1, j)
        return 0

    lax.fori_loop(0, PIECES, first, 0)
    for d in (CW, CCW):
        x_copy(d, 1).wait()
    lax.fori_loop(0, PIECES, second, 0)

    def step(k):
        def piece(j, _):
            down(k, j)
            sent(k - 1, j)
            send(k, j)

            @pl.when(j == 0)
            def _():
                for d in (CW, CCW):
                    x_copy(d, k + 1).wait()

            gate_up(lax.rem(k + 1, 2), j)
            return 0

        lax.fori_loop(0, PIECES, piece, 0)

    def middle(k, _):
        start_x(k + 1)
        step(k)
        return 0

    lax.fori_loop(1, n - 1, middle, 0)

    for g, (start, count) in enumerate(GROUPS):
        def last(j, _):
            down(n - 1, j)
            sent(n - 2, j)
            return 0

        lax.fori_loop(start, start + count, last, 0)
        for d in (CW, CCW):
            ag_copy(d, 0, g).start()

    def gather(m, forward):
        for g in range(len(GROUPS)):
            for d in (CW, CCW):
                ag_wait(d, m, g)
                if forward:
                    ag_copy(d, m, g).start()

    def gather_forward(m, _):
        gather(m, True)
        return 0

    lax.fori_loop(1, n - 1, gather_forward, 0)
    gather(n - 1, False)

    for d in (CW, CCW):
        pieces = buf.at[d, pl.ds(0, n - 1)]
        pltpu.make_async_copy(pieces, pieces, ag_send.at[d]).wait()


def unpack(n, buf, y_hbm, sem):
    half = buf.shape[2]
    for c in range(n):
        for d in (CW, CCW):
            pltpu.make_async_copy(buf.at[d, c], y_hbm.at[pl.ds((2 * c + d) * half, half)], sem).start()
    pltpu.make_async_copy(y_hbm, y_hbm, sem).wait()


def solution(mesh):
    n = mesh.shape["tp"]

    def step(x, w_gate, w_up, w_down):
        (rows, depth), width = x.shape, w_gate.shape[1]
        half = rows // n // 2
        fb, db = width // PIECES, depth // PIECES
        any_space = pl.BlockSpec(memory_space=pl.ANY)
        packed = pl.pallas_call(
            functools.partial(kernel, n),
            out_shape=pltpu.VMEM((2, n, half, depth), jnp.bfloat16),
            in_specs=[any_space] * 4,
            out_specs=pl.BlockSpec(memory_space=pltpu.VMEM),
            scratch_shapes=[
                pltpu.VMEM((PIECES, depth, 2 * fb), jnp.bfloat16),
                pltpu.VMEM((PIECES, width, db), jnp.bfloat16),
                pltpu.VMEM((2, 2 * half, depth), jnp.bfloat16),
                pltpu.VMEM((2, 2 * half, width), jnp.bfloat16),
                pltpu.SemaphoreType.DMA((2, PIECES)),
                pltpu.SemaphoreType.DMA((PIECES,)),
                pltpu.SemaphoreType.DMA((2, 2)),
                pltpu.SemaphoreType.DMA((2, 2)),
                pltpu.SemaphoreType.DMA((2, n, PIECES)),
                pltpu.SemaphoreType.DMA((2, n, len(GROUPS))),
                pltpu.SemaphoreType.DMA((2, PIECES)),
                pltpu.SemaphoreType.DMA((2,)),
            ],
            cost_estimate=pl.CostEstimate(
                flops=6 * rows * depth * width,
                bytes_accessed=2 * (3 * depth * width + rows * depth),
                transcendentals=rows * width),
            compiler_params=pltpu.CompilerParams(
                collective_id=0, has_side_effects=True, vmem_limit_bytes=50_000_000),
        )(x, w_gate, w_up, w_down)
        return pl.pallas_call(
            functools.partial(unpack, n),
            out_shape=jax.ShapeDtypeStruct((rows, depth), jnp.bfloat16),
            in_specs=[pl.BlockSpec(memory_space=pltpu.VMEM)],
            out_specs=any_space,
            scratch_shapes=[pltpu.SemaphoreType.DMA],
            compiler_params=pltpu.CompilerParams(vmem_limit_bytes=1_000_000),
        )(packed)

    return jax.shard_map(
        step,
        mesh=mesh,
        in_specs=(P("dp", None), P(None, "tp"), P(None, "tp"), P("tp", None)),
        out_specs=P("dp", None),
        check_vma=False,
    )
```
